32 devices in a mesh: group: 2 (over x), blk: 16 (over z, y, core).
Axes of the slice: x: 2, y: 2, z: 4, core: 2. Of those that a mesh axis runs over, the one named last changes fastest.
Arguments:
- spectra: bfloat16 [2, 2048, 768], P(None, ('group', 'blk')), parts along dimension 1, may hold values from -6 to 6
- gap_mask: int32 [2048, 48], P(('group', 'blk')), parts along dimension 0, may hold values 0 or 1
Outputs:
- correlation: float32 [8, 2048, 1024], P(None, ('group', 'blk')), parts along dimension 1
The draws below stay inside these ranges and needn't reach their ends.
There are 2 independent parts, one for each index of `group`. The reference program is written for one: setup_inputs(seed, part) draws one part's arguments, and reference() takes and returns one part's arrays. A program takes and returns all parts, laid end to end along the dimension named above; each array names one. Nothing has to cross between parts.
All inputs are finite; a program needn't handle non-finite values. No bound on the sum of `gap_mask` on one device may be relied on, other than what follows from the above.
Results may differ from the reference program's by a relative error of at most 0.0085.
Values may be sent and summed in bfloat16 or wider, within the bound.
No kernel may reach another device: no remote copies, remote signals or barrier semaphores. Data moves between devices by JAX's collectives and lax.ppermute only.
A program may use at most 192 MiB of HBM per device.

```python
import math
import jax
import jax.numpy as jnp
from jax import lax

STA_DEV = 64
WINDOWS = 48
BINS = 16
LAGS = 8
STATIONS = 1024
N_BLK = 16


def touch_ends(values, rng, smallest, largest):
    longest = values.shape.index(max(values.shape))
    spots = []
    for shift in (0, 1):
        where = [jax.random.randint(jax.random.fold_in(rng, axis), (), 0, length) for axis, length in enumerate(values.shape)]
        where[longest] = (where[longest] + shift) % values.shape[longest]
        spots.append(tuple(where))
    return values.at[spots[0]].set(smallest).at[spots[1]].set(largest)


def block_scale(rng, shape, split, smallest, largest):
    def one(axis_at, blocks):
        heights = jax.random.uniform(jax.random.fold_in(jax.random.fold_in(rng, 6), axis_at), (blocks,), jnp.float32, smallest / len(split), largest / len(split))
        return jnp.repeat(jnp.exp(heights), shape[axis_at] // blocks).reshape((-1,) + (1,) * (len(shape) - axis_at - 1))

    level = one(*split[0])
    for cut in split[1:]:
        level = level * one(*cut)
    return level


def bell_draw(rng, dims, deviation, most, pieces=(), held_as=jnp.bfloat16):
    entries = deviation * jax.random.normal(rng, dims, jnp.float32)
    if pieces:
        entries = entries * block_scale(rng, dims, pieces, -0.22, 0.18)
    return jnp.clip(entries, -most, most).astype(held_as)


def setup_inputs(seed: int = 0, part: int = 0) -> dict:
    splits = jax.random.split(jax.random.key(seed), 3)
    part_splits = jax.random.split(jax.random.fold_in(splits[2], part), 3)
    return {
        "spectra": bell_draw(part_splits[0], (2, STATIONS, WINDOWS * BINS), 1.0, 6.0, ((1, 16),)),
        "gap_mask": touch_ends((jax.random.randint(part_splits[1], (STATIONS, WINDOWS), 0, 8) < 7).astype(jnp.int32), jax.random.fold_in(part_splits[1], 1), 0, 1),
    }


level_floor = 0.3
first_bin = 96.0

def band_table(bin_count):
    ladder = jnp.arange(bin_count, dtype=jnp.int32)
    near = (jnp.abs(ladder[:, None] - ladder[None, :]) <= 2).astype(jnp.float32)
    return near / lax.optimization_barrier(jnp.sum(near, axis=0, keepdims=True))

def phase_tables(bin_count, lag_count):
    freq = first_bin + jnp.arange(bin_count, dtype=jnp.float32)
    shifts = 3.0 + 5.0 * jnp.arange(lag_count, dtype=jnp.float32)
    theta = 2.0 * math.pi * freq[:, None] * shifts[None, :] / 512.0
    return (jnp.cos(theta), jnp.sin(theta))

def whiten(spectra, gap_mask):
    members = spectra.shape[1]
    win_count = gap_mask.shape[1]
    bin_count = spectra.shape[2] // win_count
    parts = spectra.astype(jnp.float32).reshape(2, members, win_count, bin_count)
    amplitude = jnp.sqrt(parts[0] * parts[0] + parts[1] * parts[1])
    level = jnp.einsum('swg,gf->swf', amplitude, band_table(bin_count), precision=lax.Precision.HIGHEST)
    level = jnp.maximum(level, level_floor)
    factor = gap_mask.astype(jnp.float32)[None, :, :, None] / level[None]
    return (parts * factor).astype(jnp.bfloat16)

def modulate(whitened, lag_count):
    win_count = whitened.shape[2]
    bin_count = whitened.shape[3]
    cosine, sine = phase_tables(bin_count, lag_count)
    scale = 1.0 / math.sqrt(win_count * bin_count)
    values = whitened.astype(jnp.float32)
    cos_rows = cosine.T[:, None, None, None, :]
    sin_rows = sine.T[:, None, None, None, :]
    even_mod = (cos_rows * values[None] * scale).astype(jnp.bfloat16)
    swapped = jnp.stack([values[1], -values[0]])
    odd_mod = (sin_rows * swapped[None] * scale).astype(jnp.bfloat16)
    return jnp.stack([even_mod, odd_mod])

def reference(spectra, gap_mask):
    whitened = whiten(spectra, gap_mask)
    modulated = modulate(whitened, LAGS)
    flat_white = whitened.astype(jnp.float32).reshape(2, STATIONS, WINDOWS * BINS)

    def one_block(block_id):
        start = (block_id * STA_DEV).astype(jnp.int32)
        piece = lax.dynamic_slice_in_dim(modulated, start, STA_DEV, 3)
        piece = piece.astype(jnp.float32).reshape(2, LAGS, 2, STA_DEV, WINDOWS * BINS)
        terms = jnp.einsum('hjcsk,ctk->hjst', piece, flat_white, precision=lax.Precision.HIGHEST)
        return terms[0] - terms[1]
    blocks = lax.map(one_block, jnp.arange(N_BLK, dtype=jnp.int32))
    return jnp.transpose(blocks, (1, 0, 2, 3)).reshape(LAGS, STATIONS, STATIONS)
```

```python
import math

import numpy as np
import jax
import jax.numpy as jnp
from jax import lax
from jax.experimental import pallas as pl
from jax.experimental.pallas import tpu as pltpu
from jax.sharding import PartitionSpec as P

LAGS = 8

level_floor = 0.3
first_bin = 96.0
REACH = 2


def phase_tables(bin_count, win_count, lag_count):
    freq = first_bin + np.arange(bin_count, dtype=np.float64)
    shifts = 3.0 + 5.0 * np.arange(lag_count, dtype=np.float64)
    theta = 2.0 * math.pi * shifts[:, None] * freq[None, :] / 512.0
    scale = 1.0 / math.sqrt(win_count * bin_count)
    tables = [np.tile(part(theta) * scale, (1, win_count)) for part in (np.cos, np.sin)]
    return [jnp.asarray(t[:, None, :], jnp.float32) for t in tables]


def spread_table(bin_count, win_count):
    return jnp.asarray(np.repeat(np.eye(win_count), bin_count, axis=1), jnp.bfloat16)


def whiten_body(spectra, gap_mask, spread, out):
    wide = spectra.shape[2]
    bin_count = wide // gap_mask.shape[1]
    real = spectra[0].astype(jnp.float32)
    imag = spectra[1].astype(jnp.float32)
    amplitude = jnp.sqrt(real * real + imag * imag)
    lane = lax.broadcasted_iota(jnp.int32, amplitude.shape, 1) % bin_count
    total = amplitude
    count = jnp.ones(amplitude.shape, jnp.float32)
    for step in range(1, REACH + 1):
        above = lane + step < bin_count
        below = lane >= step
        total = total + jnp.where(above, pltpu.roll(amplitude, wide - step, 1), 0.0)
        total = total + jnp.where(below, pltpu.roll(amplitude, step, 1), 0.0)
        count = count + above.astype(jnp.float32) + below.astype(jnp.float32)
    level = jnp.maximum(total / count, level_floor)
    kept = jnp.dot(
        gap_mask[...].astype(jnp.float32).astype(jnp.bfloat16),
        spread[...],
        preferred_element_type=jnp.float32,
    )
    factor = kept / level
    out[:, :wide] = (real * factor).astype(jnp.bfloat16)
    out[:, wide:] = (imag * factor).astype(jnp.bfloat16)


def whiten(spectra, gap_mask):
    members, wide = spectra.shape[1:]
    spread = spread_table(wide // gap_mask.shape[1], gap_mask.shape[1])
    return pl.pallas_call(
        whiten_body,
        out_shape=jax.ShapeDtypeStruct((members, 2 * wide), jnp.bfloat16),
        name="whiten",
    )(spectra, gap_mask, spread)


def modulate_body(white, cosine, sine, out):
    members = white.shape[0]
    wide = white.shape[1] // 2
    real = white[:, :wide].astype(jnp.float32)
    imag = white[:, wide:].astype(jnp.float32)
    for lag in range(cosine.shape[0]):
        rows = slice(lag * members, (lag + 1) * members)
        c = cosine[lag]
        s = sine[lag]
        out[rows, :wide] = (c * real - s * imag).astype(jnp.bfloat16)
        out[rows, wide:] = (c * imag + s * real).astype(jnp.bfloat16)


def modulate(white, win_count):
    members = white.shape[0]
    cosine, sine = phase_tables(white.shape[1] // 2 // win_count, win_count, LAGS)
    return pl.pallas_call(
        modulate_body,
        out_shape=jax.ShapeDtypeStruct((LAGS * members, white.shape[1]), jnp.bfloat16),
        name="modulate",
    )(white, cosine, sine)


def correlate(where, modulated, groups, shape, onto=None):
    flat = [piece for mine, other in groups for piece in (*mine, *other)]
    chips = len(groups)
    members = shape[1]
    extra = [] if onto is None else [onto]

    def body(where, modulated, *rest):
        pieces = rest[: len(flat)]
        out, pair, tile, sems = rest[len(flat) + len(extra) :]
        core = where[0]
        copies = []
        at = 0
        for g, (mine, other) in enumerate(groups):
            for side, parts in ((core, mine), (1 - core, other)):
                rows = pl.ds(pl.multiple_of(side * members, members), members)
                left = 0
                for part in parts:
                    pair[g, rows, left : left + part.shape[1]] = pieces[at][...]
                    left += part.shape[1]
                    at += 1
            sums = lax.dot_general(
                modulated[...], pair[g], (((1,), (1,)), ((), ())), preferred_element_type=jnp.float32
            )
            tile[g] = sums.reshape(shape[0], members, 2 * members)
            first = pl.multiple_of(where[1 + g] * (2 * members), 2 * members)
            copy = pltpu.make_async_copy(tile.at[g], out.at[:, :, pl.ds(first, 2 * members)], sems.at[g])
            copy.start()
            copies.append(copy)
        for copy in copies:
            copy.wait()

    vmem = pl.BlockSpec(memory_space=pltpu.VMEM)
    anywhere = pl.BlockSpec(memory_space=pl.ANY)
    return pl.pallas_call(
        body,
        out_shape=jax.ShapeDtypeStruct(shape, jnp.float32),
        in_specs=[pl.BlockSpec(memory_space=pltpu.SMEM)] + [vmem] * (1 + len(flat)) + [anywhere] * len(extra),
        out_specs=anywhere,
        scratch_shapes=[
            pltpu.VMEM((chips, 2 * members, modulated.shape[1]), jnp.bfloat16),
            pltpu.VMEM((chips, shape[0], members, 2 * members), jnp.float32),
            pltpu.SemaphoreType.DMA((chips,)),
        ],
        input_output_aliases={} if onto is None else {2 + len(flat): 0},
        name="correlate",
    )(where, modulated, *flat, *extra)


def chip_order(chips):
    return list(range(0, chips, 2)) + list(range(1, chips, 2))[::-1]


def per_device(spectra, gap_mask):
    devices = lax.axis_size("blk")
    chips = devices // 2
    walk = chip_order(chips)
    place = lax.axis_index("blk")
    core = place % 2
    chip = place // 2
    seat = jnp.asarray(np.argsort(walk), jnp.int32)[chip]
    members = spectra.shape[1]
    win_count = gap_mask.shape[1]

    def shift(array, by):
        pairs = [
            (2 * walk[i] + c, 2 * walk[(i + by) % chips] + c) for i in range(chips) for c in range(2)
        ]
        return lax.ppermute(array, "blk", pairs)

    def swap(array):
        return lax.ppermute(array, "blk", [(i, i ^ 1) for i in range(devices)])

    white = whiten(spectra, gap_mask)
    modulated = modulate(white, win_count)
    half = white.shape[1] // 2

    up, down = white, white
    groups = [((white,), (swap(white),))]
    steps = [0]
    for step in range(1, chips // 2):
        up = shift(up, 1)
        down = shift(down, -1)
        groups.append(((up,), (swap(up),)))
        groups.append(((down,), (swap(down),)))
        steps += [-step, step]
    last_up = shift(up[:, :half], 1)
    last_down = shift(down[:, half:], -1)
    last = ((last_up, last_down), (swap(last_up), swap(last_down)))

    order = jnp.asarray(walk, jnp.int32)
    seats = (seat + jnp.asarray(steps + [chips // 2], jnp.int32)) % chips
    homes = order[seats]
    shape = (LAGS, members, devices * members)
    head = core[None].astype(jnp.int32)
    most = correlate(jnp.concatenate([head, homes[:-1]]), modulated, groups, shape)
    return correlate(jnp.concatenate([head, homes[-1:]]), modulated, [last], shape, onto=most)


def solution(mesh):
    placed = (P(None, ("group", "blk"), None), P(("group", "blk"), None))
    return jax.shard_map(
        per_device,
        mesh=mesh,
        in_specs=placed,
        out_specs=P(None, ("group", "blk"), None),
        check_vma=False,
    )
```

```python
import math

import numpy as np
import jax
import jax.numpy as jnp
from jax import lax
from jax.experimental import pallas as pl
from jax.experimental.pallas import tpu as pltpu
from jax.sharding import PartitionSpec as P


LAGS = 8

level_floor = 0.3
first_bin = 96.0
REACH = 2
ROOM = 16 * 2**20
PARTS = 2


def phase_tables(bin_count, win_count, lag_count):
    freq = first_bin + np.arange(bin_count, dtype=np.float64)
    shifts = 3.0 + 5.0 * np.arange(lag_count, dtype=np.float64)
    theta = 2.0 * math.pi * shifts[:, None] * freq[None, :] / 512.0
    scale = 1.0 / math.sqrt(win_count * bin_count)
    tables = [np.tile(part(theta) * scale, (1, win_count)) for part in (np.cos, np.sin)]
    return [jnp.asarray(t[:, None, :], jnp.float32) for t in tables]


def near(array):
    return pltpu.with_memory_space_constraint(array, pltpu.VMEM)


def far(array):
    return pltpu.with_memory_space_constraint(array, pltpu.HBM)


def whiten_body(spectra, gap_mask, out):
    wide = spectra.shape[2]
    bin_count = wide // gap_mask.shape[0]
    real = spectra[0].astype(jnp.float32)
    imag = spectra[1].astype(jnp.float32)
    amplitude = jnp.sqrt(real * real + imag * imag)
    lane = lax.broadcasted_iota(jnp.int32, amplitude.shape, 1) % bin_count
    total = amplitude
    count = jnp.ones(amplitude.shape, jnp.float32)
    for step in range(1, REACH + 1):
        above = lane + step < bin_count
        below = lane >= step
        total = total + jnp.where(above, pltpu.roll(amplitude, wide - step, 1), 0.0)
        total = total + jnp.where(below, pltpu.roll(amplitude, step, 1), 0.0)
        count = count + above.astype(jnp.float32) + below.astype(jnp.float32)
    level = jnp.maximum(total / count, level_floor)
    window = lax.broadcasted_iota(jnp.int32, (gap_mask.shape[0], wide), 1) // bin_count
    spread = window == lax.broadcasted_iota(jnp.int32, window.shape, 0)
    kept = lax.dot_general(
        gap_mask[...].astype(jnp.float32).astype(jnp.bfloat16),
        spread.astype(jnp.float32).astype(jnp.bfloat16),
        (((0,), (0,)), ((), ())),
        preferred_element_type=jnp.float32,
    )
    factor = kept / level
    out[:, :wide] = (real * factor).astype(jnp.bfloat16)
    out[:, wide:] = (imag * factor).astype(jnp.bfloat16)


def whiten(spectra, gap_mask):
    members, wide = spectra.shape[1:]
    return pl.pallas_call(
        whiten_body,
        out_shape=pltpu.VMEM((members, 2 * wide), jnp.bfloat16),
        compiler_params=pltpu.CompilerParams(vmem_limit_bytes=ROOM),
        name="whiten",
    )(far(spectra), far(gap_mask.T))


def modulate_body(white, cosine, sine, out):
    members = white.shape[0]
    wide = white.shape[1] // 2
    real = white[:, :wide].astype(jnp.float32)
    imag = white[:, wide:].astype(jnp.float32)
    for lag in range(cosine.shape[0]):
        rows = slice(lag * members, (lag + 1) * members)
        c = cosine[lag]
        s = sine[lag]
        out[rows, :wide] = (c * real - s * imag).astype(jnp.bfloat16)
        out[rows, wide:] = (c * imag + s * real).astype(jnp.bfloat16)


def modulate(white, win_count):
    members = white.shape[0]
    cosine, sine = phase_tables(white.shape[1] // 2 // win_count, win_count, LAGS)
    return pl.pallas_call(
        modulate_body,
        out_shape=pltpu.VMEM((LAGS * members, white.shape[1]), jnp.bfloat16),
        compiler_params=pltpu.CompilerParams(vmem_limit_bytes=ROOM),
        cost_estimate=pl.CostEstimate(flops=12 * LAGS * white.size, bytes_accessed=0, transcendentals=0),
        name="modulate",
    )(near(white), cosine, sine)


def walk_at(seat, chips):
    return jnp.where(seat < chips // 2, 2 * seat, 2 * (chips - 1 - seat) + 1)


def seat_of(chip, chips):
    return jnp.where(chip % 2 == 0, chip // 2, chips - 1 - chip // 2)


def correlate(modulated, groups, chips, shape, onto=None):
    flat = [piece for _, mine, other in groups for piece in (*mine, *other)]
    members = shape[1]
    extra = [] if onto is None else [onto]
    count = len(groups)

    def body(modulated, *rest):
        pieces = rest[: len(flat)]
        out, block, tile, sems = rest[len(flat) + len(extra) :]
        place = lax.axis_index("blk")
        core = lax.rem(place, 2)
        seat = seat_of(lax.div(place, 2), chips)
        at = 0
        for g, (_, mine, other) in enumerate(groups):
            for side, parts in ((core, mine), (1 - core, other)):
                rows = pl.ds(pl.multiple_of((2 * g + side) * members, members), members)
                left = 0
                for part in parts:
                    block[rows, left : left + part.shape[1]] = pieces[at][...]
                    left += part.shape[1]
                    at += 1
        copies = []
        lags = shape[0] // PARTS
        for part in range(PARTS):
            sums = lax.dot_general(
                modulated[part * lags * members : (part + 1) * lags * members, :],
                block[...],
                (((1,), (1,)), ((), ())),
                preferred_element_type=jnp.float32,
            ).reshape(lags, members, 2 * count * members)
            some = pl.ds(part * lags, lags)
            for g, (ahead, _, _) in enumerate(groups):
                tile[g, some] = sums[:, :, 2 * g * members : 2 * (g + 1) * members]
                home = walk_at(lax.rem(seat + ahead + chips, chips), chips)
                columns = pl.ds(pl.multiple_of(home * (2 * members), 2 * members), 2 * members)
                copy = pltpu.make_async_copy(
                    tile.at[g, some], out.at[some, :, columns], sems.at[g, part]
                )
                copy.start()
                copies.append(copy)
        for copy in copies:
            copy.wait()

    vmem = pl.BlockSpec(memory_space=pltpu.VMEM)
    anywhere = pl.BlockSpec(memory_space=pl.ANY)
    return pl.pallas_call(
        body,
        out_shape=jax.ShapeDtypeStruct(shape, jnp.float32),
        in_specs=[vmem] * (1 + len(flat)) + [anywhere] * len(extra),
        out_specs=anywhere,
        scratch_shapes=[
            pltpu.VMEM((count * 2 * members, modulated.shape[1]), jnp.bfloat16),
            pltpu.VMEM((count, shape[0], members, 2 * members), jnp.float32),
            pltpu.SemaphoreType.DMA((count, PARTS)),
        ],
        input_output_aliases={} if onto is None else {1 + len(flat): 0},
        compiler_params=pltpu.CompilerParams(vmem_limit_bytes=ROOM),
        cost_estimate=pl.CostEstimate(
            flops=4 * count * members * modulated.size, bytes_accessed=0, transcendentals=0
        ),
        name="correlate",
    )(near(modulated), *[near(piece) for piece in flat], *extra)


def per_device(spectra, gap_mask):
    devices = lax.axis_size("blk")
    chips = devices // 2
    walk = list(range(0, chips, 2)) + list(range(1, chips, 2))[::-1]
    members = spectra.shape[1]
    shape = (LAGS, members, devices * members)

    def shift(array, by):
        pairs = [
            (2 * walk[i] + c, 2 * walk[(i + by) % chips] + c) for i in range(chips) for c in range(2)
        ]
        return lax.ppermute(array, "blk", pairs)

    def swap(array):
        return lax.ppermute(array, "blk", [(i, i ^ 1) for i in range(devices)])

    def add(groups, out):
        return correlate(modulated, groups, chips, shape, onto=out)

    white = whiten(spectra, gap_mask)
    modulated = modulate(white, gap_mask.shape[1])
    half = white.shape[1] // 2

    up, down = white, white
    out = add([(0, (white,), (swap(white),))], None)
    final = chips // 2
    for step in range(1, final):
        up = shift(up, 1)
        down = shift(down, -1)
        groups = [(-step, (up,), (swap(up),)), (step, (down,), (swap(down),))]
        out = add(groups, out)
    up = shift(up[:, :half], 1)
    down = shift(down[:, half:], -1)
    last = (final, (up, down), (swap(up), swap(down)))
    return add([last], out)


def solution(mesh):
    placed = (P(None, ("group", "blk"), None), P(("group", "blk"), None))
    return jax.shard_map(
        per_device,
        mesh=mesh,
        in_specs=placed,
        out_specs=P(None, ("group", "blk"), None),
        check_vma=False,
    )
```

```python
import math

import numpy as np
import jax
import jax.numpy as jnp
from jax import lax
from jax.experimental import pallas as pl
from jax.experimental.pallas import tpu as pltpu
from jax.sharding import PartitionSpec as P


LAGS = 8

level_floor = 0.3
first_bin = 96.0
REACH = 2
ROOM = 16 * 2**20
PARTS = 2


def phase_tables(bin_count, win_count, lag_count):
    freq = first_bin + np.arange(bin_count, dtype=np.float64)
    shifts = 3.0 + 5.0 * np.arange(lag_count, dtype=np.float64)
    theta = 2.0 * math.pi * shifts[:, None] * freq[None, :] / 512.0
    scale = 1.0 / math.sqrt(win_count * bin_count)
    tables = [np.tile(part(theta) * scale, (1, win_count)) for part in (np.cos, np.sin)]
    return [jnp.asarray(t[:, None, :], jnp.float32) for t in tables]


def near(array):
    return pltpu.with_memory_space_constraint(array, pltpu.VMEM)


def far(array):
    return pltpu.with_memory_space_constraint(array, pltpu.HBM)


def whiten_body(spectra, gap_mask, out):
    wide = spectra.shape[2]
    bin_count = wide // gap_mask.shape[0]
    real = spectra[0].astype(jnp.float32)
    imag = spectra[1].astype(jnp.float32)
    amplitude = jnp.sqrt(real * real + imag * imag)
    lane = lax.broadcasted_iota(jnp.int32, amplitude.shape, 1) % bin_count
    total = amplitude
    count = jnp.ones(amplitude.shape, jnp.float32)
    for step in range(1, REACH + 1):
        above = lane + step < bin_count
        below = lane >= step
        total = total + jnp.where(above, pltpu.roll(amplitude, wide - step, 1), 0.0)
        total = total + jnp.where(below, pltpu.roll(amplitude, step, 1), 0.0)
        count = count + above.astype(jnp.float32) + below.astype(jnp.float32)
    level = jnp.maximum(total / count, level_floor)
    window = lax.broadcasted_iota(jnp.int32, (gap_mask.shape[0], wide), 1) // bin_count
    spread = window == lax.broadcasted_iota(jnp.int32, window.shape, 0)
    kept = lax.dot_general(
        gap_mask[...].astype(jnp.float32).astype(jnp.bfloat16),
        spread.astype(jnp.float32).astype(jnp.bfloat16),
        (((0,), (0,)), ((), ())),
        preferred_element_type=jnp.float32,
    )
    factor = kept / level
    out[:, :wide] = (real * factor).astype(jnp.bfloat16)
    out[:, wide:] = (imag * factor).astype(jnp.bfloat16)


def whiten(spectra, gap_mask):
    members, wide = spectra.shape[1:]
    return pl.pallas_call(
        whiten_body,
        out_shape=pltpu.VMEM((members, 2 * wide), jnp.bfloat16),
        compiler_params=pltpu.CompilerParams(vmem_limit_bytes=ROOM),
        name="whiten",
    )(far(spectra), far(gap_mask.T))


def modulate_body(white, cosine, sine, out):
    members = white.shape[0]
    wide = white.shape[1] // 2
    real = white[:, :wide].astype(jnp.float32)
    imag = white[:, wide:].astype(jnp.float32)
    for lag in range(cosine.shape[0]):
        rows = slice(lag * members, (lag + 1) * members)
        c = cosine[lag]
        s = sine[lag]
        out[rows, :wide] = (c * real - s * imag).astype(jnp.bfloat16)
        out[rows, wide:] = (c * imag + s * real).astype(jnp.bfloat16)


def modulate(white, win_count):
    members = white.shape[0]
    cosine, sine = phase_tables(white.shape[1] // 2 // win_count, win_count, LAGS)
    return pl.pallas_call(
        modulate_body,
        out_shape=pltpu.VMEM((LAGS * members, white.shape[1]), jnp.bfloat16),
        compiler_params=pltpu.CompilerParams(vmem_limit_bytes=ROOM),
        cost_estimate=pl.CostEstimate(flops=12 * LAGS * white.size, bytes_accessed=0, transcendentals=0),
        name="modulate",
    )(near(white), cosine, sine)


def walk_at(seat, chips):
    return jnp.where(seat < chips // 2, 2 * seat, 2 * (chips - 1 - seat) + 1)


def seat_of(chip, chips):
    return jnp.where(chip % 2 == 0, chip // 2, chips - 1 - chip // 2)


def correlate(modulated, groups, chips, shape, onto=None):
    flat = [piece for _, mine, other in groups for piece in (mine, other)]
    members = shape[1]
    extra = [] if onto is None else [onto]
    count = len(groups)

    def body(modulated, *rest):
        pieces = rest[: len(flat)]
        out, block, tile, sems = rest[len(flat) + len(extra) :]
        place = lax.axis_index("blk")
        core = lax.rem(place, 2)
        seat = seat_of(lax.div(place, 2), chips)
        for g in range(count):
            for side, piece in ((core, pieces[2 * g]), (1 - core, pieces[2 * g + 1])):
                rows = pl.ds(pl.multiple_of((2 * g + side) * members, members), members)
                block[rows, :] = piece[...]
        copies = []
        lags = shape[0] // PARTS
        for part in range(PARTS):
            sums = lax.dot_general(
                modulated[part * lags * members : (part + 1) * lags * members, :],
                block[...],
                (((1,), (1,)), ((), ())),
                preferred_element_type=jnp.float32,
            ).reshape(lags, members, 2 * count * members)
            some = pl.ds(part * lags, lags)
            for g, (back, _, _) in enumerate(groups):
                tile[g, some] = sums[:, :, 2 * g * members : 2 * (g + 1) * members]
                home = walk_at(lax.rem(seat + chips - back * (1 - 2 * core), chips), chips)
                columns = pl.ds(pl.multiple_of(home * (2 * members), 2 * members), 2 * members)
                copy = pltpu.make_async_copy(
                    tile.at[g, some], out.at[some, :, columns], sems.at[g, part]
                )
                copy.start()
                copies.append(copy)
        for copy in copies:
            copy.wait()

    vmem = pl.BlockSpec(memory_space=pltpu.VMEM)
    anywhere = pl.BlockSpec(memory_space=pl.ANY)
    return pl.pallas_call(
        body,
        out_shape=jax.ShapeDtypeStruct(shape, jnp.float32),
        in_specs=[vmem] * (1 + len(flat)) + [anywhere] * len(extra),
        out_specs=anywhere,
        scratch_shapes=[
            pltpu.VMEM((count * 2 * members, modulated.shape[1]), jnp.bfloat16),
            pltpu.VMEM((count, shape[0], members, 2 * members), jnp.float32),
            pltpu.SemaphoreType.DMA((count, PARTS)),
        ],
        input_output_aliases={} if onto is None else {1 + len(flat): 0},
        compiler_params=pltpu.CompilerParams(vmem_limit_bytes=ROOM),
        cost_estimate=pl.CostEstimate(
            flops=4 * count * members * modulated.size, bytes_accessed=0, transcendentals=0
        ),
        name="correlate",
    )(near(modulated), *[near(piece) for piece in flat], *extra)


def per_device(spectra, gap_mask):
    devices = lax.axis_size("blk")
    chips = devices // 2
    walk = list(range(0, chips, 2)) + list(range(1, chips, 2))[::-1]
    members = spectra.shape[1]
    shape = (LAGS, members, devices * members)

    def onward(array):
        pairs = [
            (2 * walk[i] + c, 2 * walk[(i + 1 - 2 * c) % chips] + c) for i in range(chips) for c in range(2)
        ]
        return lax.ppermute(array, "blk", pairs)

    def swap(array):
        return lax.ppermute(array, "blk", [(i, i ^ 1) for i in range(devices)])

    def add(groups, out):
        return correlate(modulated, groups, chips, shape, onto=out)

    white = whiten(spectra, gap_mask)
    modulated = modulate(white, gap_mask.shape[1])

    mine, other = white, swap(white)
    out = add([(0, mine, other)], None)
    final = chips // 2
    waiting = []
    for step in range(1, final):
        mine = onward(mine)
        other = onward(other)
        out = add([(step, mine, other)] + waiting, out)
        waiting = [(-step, swap(other), swap(mine))]
    mine = onward(mine)
    out = add(waiting, out)
    return add([(final, mine, swap(mine))], out)


def solution(mesh):
    placed = (P(None, ("group", "blk"), None), P(("group", "blk"), None))
    return jax.shard_map(
        per_device,
        mesh=mesh,
        in_specs=placed,
        out_specs=P(None, ("group", "blk"), None),
        check_vma=False,
    )
```

```python
import math

import numpy as np
import jax
import jax.numpy as jnp
from jax import lax
from jax.experimental import pallas as pl
from jax.experimental.pallas import tpu as pltpu
from jax.sharding import PartitionSpec as P


LAGS = 8

level_floor = 0.3
first_bin = 96.0
REACH = 2
ROOM = 16 * 2**20
PARTS = 2


def phase_tables(bin_count, win_count, lag_count):
    freq = first_bin + np.arange(bin_count, dtype=np.float64)
    shifts = 3.0 + 5.0 * np.arange(lag_count, dtype=np.float64)
    theta = 2.0 * math.pi * shifts[:, None] * freq[None, :] / 512.0
    scale = 1.0 / math.sqrt(win_count * bin_count)
    tables = [np.tile(part(theta) * scale, (1, win_count)) for part in (np.cos, np.sin)]
    return jnp.asarray(np.concatenate(tables), jnp.float32)


def near(array):
    return pltpu.with_memory_space_constraint(array, pltpu.VMEM)


def far(array):
    return pltpu.with_memory_space_constraint(array, pltpu.HBM)


def whiten_body(spectra, gap_mask, tables, out, tables_near):
    tables_near[...] = tables[...]
    wide = spectra.shape[2]
    bin_count = wide // gap_mask.shape[0]
    real = spectra[0].astype(jnp.float32)
    imag = spectra[1].astype(jnp.float32)
    amplitude = jnp.sqrt(real * real + imag * imag)
    lane = lax.broadcasted_iota(jnp.int32, amplitude.shape, 1) % bin_count
    total = amplitude
    count = jnp.ones(amplitude.shape, jnp.float32)
    for step in range(1, REACH + 1):
        above = lane + step < bin_count
        below = lane >= step
        total = total + jnp.where(above, pltpu.roll(amplitude, wide - step, 1), 0.0)
        total = total + jnp.where(below, pltpu.roll(amplitude, step, 1), 0.0)
        count = count + above.astype(jnp.float32) + below.astype(jnp.float32)
    level = jnp.maximum(total / count, level_floor)
    window = lax.broadcasted_iota(jnp.int32, (gap_mask.shape[0], wide), 1) // bin_count
    spread = window == lax.broadcasted_iota(jnp.int32, window.shape, 0)
    kept = lax.dot_general(
        gap_mask[...].astype(jnp.float32).astype(jnp.bfloat16),
        spread.astype(jnp.float32).astype(jnp.bfloat16),
        (((0,), (0,)), ((), ())),
        preferred_element_type=jnp.float32,
    )
    factor = kept / level
    out[:, :wide] = (real * factor).astype(jnp.bfloat16)
    out[:, wide:] = (imag * factor).astype(jnp.bfloat16)


def whiten(spectra, gap_mask):
    members, wide = spectra.shape[1:]
    win_count = gap_mask.shape[1]
    tables = phase_tables(wide // win_count, win_count, LAGS)
    return pl.pallas_call(
        whiten_body,
        out_shape=[
            pltpu.VMEM((members, 2 * wide), jnp.bfloat16),
            pltpu.VMEM(tables.shape, jnp.float32),
        ],
        compiler_params=pltpu.CompilerParams(vmem_limit_bytes=ROOM),
        name="whiten",
    )(far(spectra), far(gap_mask.T), far(tables))


def modulate_body(white, tables, out):
    members = white.shape[0]
    wide = white.shape[1] // 2
    real = white[:, :wide].astype(jnp.float32)
    imag = white[:, wide:].astype(jnp.float32)
    lags = tables.shape[0] // 2
    for lag in range(lags):
        rows = slice(lag * members, (lag + 1) * members)
        c = tables[lag : lag + 1, :]
        s = tables[lags + lag : lags + lag + 1, :]
        out[rows, :wide] = (c * real - s * imag).astype(jnp.bfloat16)
        out[rows, wide:] = (c * imag + s * real).astype(jnp.bfloat16)


def modulate(white, tables):
    members = white.shape[0]
    return pl.pallas_call(
        modulate_body,
        out_shape=pltpu.VMEM((LAGS * members, white.shape[1]), jnp.bfloat16),
        compiler_params=pltpu.CompilerParams(vmem_limit_bytes=ROOM),
        cost_estimate=pl.CostEstimate(flops=12 * LAGS * white.size, bytes_accessed=0, transcendentals=0),
        name="modulate",
    )(near(white), near(tables))


def walk_at(seat, chips):
    return jnp.where(seat < chips // 2, 2 * seat, 2 * (chips - 1 - seat) + 1)


def seat_of(chip, chips):
    return jnp.where(chip % 2 == 0, chip // 2, chips - 1 - chip // 2)


def correlate(modulated, groups, chips, shape, before, end):
    members = shape[1]
    count = len(groups)
    flat = [piece for _, mine, other in groups for piece in (mine, other)]
    old_groups, old_tiles, onto = before if before else ([], None, None)
    olds = ([] if old_tiles is None else [old_tiles]) + ([] if onto is None else [onto])

    def body(modulated, *rest):
        pieces = rest[: len(flat)]
        old_tile = rest[len(flat)]
        tail = rest[len(flat) + len(olds) :]
        if end:
            out, block, sems, tile = tail
        elif old_groups:
            tile, out, block, sems = tail
        else:
            tile, block, sems = tail
        place = lax.axis_index("blk")
        core = lax.rem(place, 2)
        seat = seat_of(lax.div(place, 2), chips)
        copies = []

        def send(source, back, some, sem):
            home = walk_at(lax.rem(seat + chips - back * (1 - 2 * core), chips), chips)
            columns = pl.ds(pl.multiple_of(home * (2 * members), 2 * members), 2 * members)
            copy = pltpu.make_async_copy(source, out.at[some, :, columns], sem)
            copy.start()
            copies.append(copy)

        for g, (back, _, _) in enumerate(old_groups):
            send(old_tile.at[g], back, slice(None), sems.at[g, PARTS])
        for g in range(count):
            for side, piece in ((core, pieces[2 * g]), (1 - core, pieces[2 * g + 1])):
                rows = pl.ds(pl.multiple_of((2 * g + side) * members, members), members)
                block[rows, :] = piece[...]
        parts = PARTS if end else 1
        lags = shape[0] // parts
        for part in range(parts):
            some = pl.ds(part * lags, lags)
            sums = lax.dot_general(
                modulated[part * lags * members : (part + 1) * lags * members, :],
                block[...],
                (((1,), (1,)), ((), ())),
                preferred_element_type=jnp.float32,
            ).reshape(lags, members, 2 * count * members)
            for g, (back, _, _) in enumerate(groups):
                tile[g, some] = sums[:, :, 2 * g * members : 2 * (g + 1) * members]
                if end:
                    send(tile.at[g, some], back, some, sems.at[g, part])
        for copy in copies:
            copy.wait()

    vmem = pl.BlockSpec(memory_space=pltpu.VMEM)
    anywhere = pl.BlockSpec(memory_space=pl.ANY)
    tile_shape = (count, shape[0], members, 2 * members)
    outs = [] if end else [(pltpu.VMEM(tile_shape, jnp.float32), vmem)]
    if old_groups:
        outs.append((jax.ShapeDtypeStruct(shape, jnp.float32), anywhere))
    scratch = [
        pltpu.VMEM((count * 2 * members, modulated.shape[1]), jnp.bfloat16),
        pltpu.SemaphoreType.DMA((max(count, len(old_groups)), PARTS + 1)),
    ]
    got = pl.pallas_call(
        body,
        out_shape=[shaped for shaped, _ in outs],
        in_specs=[vmem] * (1 + len(flat)) + [vmem] * (old_tiles is not None) + [anywhere] * (onto is not None),
        out_specs=[spec for _, spec in outs],
        scratch_shapes=scratch + ([pltpu.VMEM(tile_shape, jnp.float32)] if end else []),
        input_output_aliases={} if onto is None else {2 + len(flat): len(outs) - 1},
        compiler_params=pltpu.CompilerParams(vmem_limit_bytes=ROOM),
        cost_estimate=pl.CostEstimate(
            flops=4 * count * members * modulated.size, bytes_accessed=0, transcendentals=0
        ),
        name="correlate",
    )(
        near(modulated),
        *[near(piece) for piece in flat],
        *([] if old_tiles is None else [near(old_tiles)]),
        *([] if onto is None else [onto]),
    )
    if end:
        return got[0]
    return groups, got[0], got[1] if old_groups else None


def per_device(spectra, gap_mask):
    devices = lax.axis_size("blk")
    chips = devices // 2
    walk = list(range(0, chips, 2)) + list(range(1, chips, 2))[::-1]
    members = spectra.shape[1]
    shape = (LAGS, members, devices * members)

    def onward(array, step):
        pairs = [
            (2 * walk[i] + (c + step + 1) % 2, 2 * walk[(i + 1 - 2 * c) % chips] + (c + step) % 2)
            for i in range(chips)
            for c in range(2)
        ]
        return lax.ppermute(array, "blk", pairs)

    def swap(array):
        return lax.ppermute(array, "blk", [(i, i ^ 1) for i in range(devices)])

    def add(groups, before, end=False):
        return correlate(modulated, groups, chips, shape, before, end)

    white, tables = whiten(spectra, gap_mask)
    modulated = modulate(white, tables)

    mine, other = white, swap(white)
    out = add([(0, mine, other)], None)
    final = chips // 2
    for step in range(1, final):
        mine = onward(mine, step)
        other = onward(other, step)
        mine_there, other_there = swap(mine), swap(other)
        if step % 2:
            groups = [(-step, other, mine), (step, mine_there, other_there)]
        else:
            groups = [(step, mine, other), (-step, other_there, mine_there)]
        out = add(groups, out)
    last = onward(mine, final)
    there = swap(last)
    return add([(final, there, last) if final % 2 else (final, last, there)], out, end=True)


def solution(mesh):
    placed = (P(None, ("group", "blk"), None), P(("group", "blk"), None))
    return jax.shard_map(
        per_device,
        mesh=mesh,
        in_specs=placed,
        out_specs=P(None, ("group", "blk"), None),
        check_vma=False,
    )
```

```python
import math

import numpy as np
import jax
import jax.numpy as jnp
from jax import lax
from jax.experimental import pallas as pl
from jax.experimental.pallas import tpu as pltpu
from jax.sharding import PartitionSpec as P


LAGS = 8

level_floor = 0.3
first_bin = 96.0
REACH = 2
ROOM = 16 * 2**20
PARTS = 2


def phase_tables(bin_count, win_count, lag_count):
    freq = first_bin + np.arange(bin_count, dtype=np.float64)
    shifts = 3.0 + 5.0 * np.arange(lag_count, dtype=np.float64)
    theta = 2.0 * math.pi * shifts[:, None] * freq[None, :] / 512.0
    scale = 1.0 / math.sqrt(win_count * bin_count)
    tables = [np.tile(part(theta) * scale, (1, win_count)) for part in (np.cos, np.sin)]
    return jnp.asarray(np.concatenate(tables), jnp.float32)


def near(array):
    return pltpu.with_memory_space_constraint(array, pltpu.VMEM)


def far(array):
    return pltpu.with_memory_space_constraint(array, pltpu.HBM)


def whiten_body(spectra, gap_mask, tables, out, tables_near):
    tables_near[...] = tables[...]
    wide = spectra.shape[2]
    bin_count = wide // gap_mask.shape[0]
    real = spectra[0].astype(jnp.float32)
    imag = spectra[1].astype(jnp.float32)
    amplitude = jnp.sqrt(real * real + imag * imag)
    lane = lax.broadcasted_iota(jnp.int32, amplitude.shape, 1) % bin_count
    total = amplitude
    count = jnp.ones(amplitude.shape, jnp.float32)
    for step in range(1, REACH + 1):
        above = lane + step < bin_count
        below = lane >= step
        total = total + jnp.where(above, pltpu.roll(amplitude, wide - step, 1), 0.0)
        total = total + jnp.where(below, pltpu.roll(amplitude, step, 1), 0.0)
        count = count + above.astype(jnp.float32) + below.astype(jnp.float32)
    level = jnp.maximum(total / count, level_floor)
    window = lax.broadcasted_iota(jnp.int32, (gap_mask.shape[0], wide), 1) // bin_count
    spread = window == lax.broadcasted_iota(jnp.int32, window.shape, 0)
    kept = lax.dot_general(
        gap_mask[...].astype(jnp.float32).astype(jnp.bfloat16),
        spread.astype(jnp.float32).astype(jnp.bfloat16),
        (((0,), (0,)), ((), ())),
        preferred_element_type=jnp.float32,
    )
    factor = kept / level
    out[:, :wide] = (real * factor).astype(jnp.bfloat16)
    out[:, wide:] = (imag * factor).astype(jnp.bfloat16)


def whiten(spectra, gap_mask):
    members, wide = spectra.shape[1:]
    win_count = gap_mask.shape[1]
    tables = phase_tables(wide // win_count, win_count, LAGS)
    return pl.pallas_call(
        whiten_body,
        out_shape=[
            pltpu.VMEM((members, 2 * wide), jnp.bfloat16),
            pltpu.VMEM(tables.shape, jnp.float32),
        ],
        compiler_params=pltpu.CompilerParams(vmem_limit_bytes=ROOM),
        name="whiten",
    )(far(spectra), far(gap_mask.T), far(tables))


def modulate_body(white, tables, out):
    members = white.shape[0]
    wide = white.shape[1] // 2
    real = white[:, :wide].astype(jnp.float32)
    imag = white[:, wide:].astype(jnp.float32)
    lags = tables.shape[0] // 2
    for lag in range(lags):
        rows = slice(lag * members, (lag + 1) * members)
        c = tables[lag : lag + 1, :]
        s = tables[lags + lag : lags + lag + 1, :]
        out[rows, :wide] = (c * real - s * imag).astype(jnp.bfloat16)
        out[rows, wide:] = (c * imag + s * real).astype(jnp.bfloat16)


def modulate(white, tables):
    members = white.shape[0]
    return pl.pallas_call(
        modulate_body,
        out_shape=pltpu.VMEM((LAGS * members, white.shape[1]), jnp.bfloat16),
        compiler_params=pltpu.CompilerParams(vmem_limit_bytes=ROOM),
        cost_estimate=pl.CostEstimate(flops=12 * LAGS * white.size, bytes_accessed=0, transcendentals=0),
        name="modulate",
    )(near(white), near(tables))


def walk_at(seat, chips):
    return jnp.where(seat < chips // 2, 2 * seat, 2 * (chips - 1 - seat) + 1)


def seat_of(chip, chips):
    return jnp.where(chip % 2 == 0, chip // 2, chips - 1 - chip // 2)


def correlate(modulated, groups, chips, shape, old=(), onto=None, end=False):
    members = shape[1]
    count = len(groups)
    flat = [piece for _, mine, other in groups for piece in (mine, other)]
    old_tiles = [tiles for _, tiles in old]
    first_onto = 1 + len(flat) + len(old_tiles)

    def body(modulated, *rest):
        pieces = rest[: len(flat)]
        old_refs = rest[len(flat) : len(flat) + len(old)]
        tail = rest[len(flat) + len(old) + (onto is not None) :]
        if end:
            out, block, sems, tile = tail
        elif old:
            tile, out, block, sems = tail
        else:
            tile, block, sems = tail
        place = lax.axis_index("blk")
        core = lax.rem(place, 2)
        seat = seat_of(lax.div(place, 2), chips)
        copies = []

        def send(source, back, some):
            home = walk_at(lax.rem(seat + chips - back * (1 - 2 * core), chips), chips)
            columns = pl.ds(pl.multiple_of(home * (2 * members), 2 * members), 2 * members)
            copy = pltpu.make_async_copy(source, out.at[some, :, columns], sems.at[len(copies)])
            copy.start()
            copies.append(copy)

        for (old_groups, _), old_tile in zip(old, old_refs):
            for g, (back, _, _) in enumerate(old_groups):
                send(old_tile.at[g], back, slice(None))
        for g in range(count):
            for side, piece in ((core, pieces[2 * g]), (1 - core, pieces[2 * g + 1])):
                rows = pl.ds(pl.multiple_of((2 * g + side) * members, members), members)
                block[rows, :] = piece[...]
        parts = PARTS if end else 1
        lags = shape[0] // parts
        for part in range(parts):
            some = pl.ds(part * lags, lags)
            sums = lax.dot_general(
                modulated[part * lags * members : (part + 1) * lags * members, :],
                block[...],
                (((1,), (1,)), ((), ())),
                preferred_element_type=jnp.float32,
            ).reshape(lags, members, 2 * count * members)
            for g, (back, _, _) in enumerate(groups):
                tile[g, some] = sums[:, :, 2 * g * members : 2 * (g + 1) * members]
                if end:
                    send(tile.at[g, some], back, some)
        for copy in copies:
            copy.wait()

    vmem = pl.BlockSpec(memory_space=pltpu.VMEM)
    anywhere = pl.BlockSpec(memory_space=pl.ANY)
    tile_shape = (count, shape[0], members, 2 * members)
    outs = [] if end else [(pltpu.VMEM(tile_shape, jnp.float32), vmem)]
    if old or end:
        outs.append((jax.ShapeDtypeStruct(shape, jnp.float32), anywhere))
    scratch = [
        pltpu.VMEM((count * 2 * members, modulated.shape[1]), jnp.bfloat16),
        pltpu.SemaphoreType.DMA((max(1, sum(len(old_groups) for old_groups, _ in old) + count * PARTS),)),
    ]
    got = pl.pallas_call(
        body,
        out_shape=[shaped for shaped, _ in outs],
        in_specs=[vmem] * first_onto + [anywhere] * (onto is not None),
        out_specs=[spec for _, spec in outs],
        scratch_shapes=scratch + ([pltpu.VMEM(tile_shape, jnp.float32)] if end else []),
        input_output_aliases={} if onto is None else {first_onto: len(outs) - 1},
        compiler_params=pltpu.CompilerParams(vmem_limit_bytes=ROOM),
        cost_estimate=pl.CostEstimate(
            flops=4 * count * members * modulated.size, bytes_accessed=0, transcendentals=0
        ),
        name="correlate",
    )(
        near(modulated),
        *[near(piece) for piece in flat],
        *[near(tiles) for tiles in old_tiles],
        *([] if onto is None else [onto]),
    )
    return got[0] if len(got) == 1 else got


def per_device(spectra, gap_mask):
    devices = lax.axis_size("blk")
    chips = devices // 2
    walk = list(range(0, chips, 2)) + list(range(1, chips, 2))[::-1]
    members = spectra.shape[1]
    shape = (LAGS, members, devices * members)

    def onward(array, step):
        pairs = [
            (2 * walk[i] + (c + step + 1) % 2, 2 * walk[(i + 1 - 2 * c) % chips] + (c + step) % 2)
            for i in range(chips)
            for c in range(2)
        ]
        return lax.ppermute(array, "blk", pairs)

    def swap(array):
        return lax.ppermute(array, "blk", [(i, i ^ 1) for i in range(devices)])

    def add(groups, **how):
        return correlate(modulated, groups, chips, shape, **how)

    white, tables = whiten(spectra, gap_mask)
    modulated = modulate(white, tables)

    mine, other = white, swap(white)
    groups = [(0, mine, other)]
    kept = [(groups, add(groups))]
    final = chips // 2
    for step in range(1, final):
        mine = onward(mine, step)
        other = onward(other, step)
        mine_there, other_there = swap(mine), swap(other)
        if step % 2:
            groups = [(-step, other, mine), (step, mine_there, other_there)]
        else:
            groups = [(step, mine, other), (-step, other_there, mine_there)]
        if step + 1 < final:
            kept.append((groups, add(groups)))
    tiles, out = add(groups[:1], old=kept)
    tiles, out = add(groups[1:], old=[(groups[:1], tiles)], onto=out)
    last = onward(mine, final)
    there = swap(last)
    ends = [(final, there, last) if final % 2 else (final, last, there)]
    return add(ends, old=[(groups[1:], tiles)], onto=out, end=True)


def solution(mesh):
    placed = (P(None, ("group", "blk"), None), P(("group", "blk"), None))
    return jax.shard_map(
        per_device,
        mesh=mesh,
        in_specs=placed,
        out_specs=P(None, ("group", "blk"), None),
        check_vma=False,
    )
```

```python
import math

import numpy as np
import jax
import jax.numpy as jnp
from jax import lax
from jax.experimental import pallas as pl
from jax.experimental.pallas import tpu as pltpu
from jax.sharding import PartitionSpec as P


LAGS = 8

level_floor = 0.3
first_bin = 96.0
REACH = 2
ROOM = 16 * 2**20
PARTS = 2


def phase_tables(bin_count, win_count, lag_count):
    freq = first_bin + np.arange(bin_count, dtype=np.float64)
    shifts = 3.0 + 5.0 * np.arange(lag_count, dtype=np.float64)
    theta = 2.0 * math.pi * shifts[:, None] * freq[None, :] / 512.0
    scale = 1.0 / math.sqrt(win_count * bin_count)
    tables = [np.tile(part(theta) * scale, (1, win_count)) for part in (np.cos, np.sin)]
    return jnp.asarray(np.concatenate(tables), jnp.float32)


def near(array):
    return pltpu.with_memory_space_constraint(array, pltpu.VMEM)


def far(array):
    return pltpu.with_memory_space_constraint(array, pltpu.HBM)


def whiten_body(spectra_far, gap_mask_far, tables_far, out, tables, spectra, gap_mask, sems):
    copies = [
        pltpu.make_async_copy(source, target, sems.at[i])
        for i, (source, target) in enumerate(
            ((gap_mask_far, gap_mask), (spectra_far, spectra), (tables_far, tables))
        )
    ]
    for copy in copies:
        copy.start()
    wide = spectra.shape[2]
    bin_count = wide // gap_mask.shape[0]
    lane = lax.broadcasted_iota(jnp.int32, (8, wide), 1) % bin_count
    count = jnp.ones(lane.shape, jnp.float32)
    keeps = []
    for step in range(1, REACH + 1):
        for keep, by in ((lane + step < bin_count, wide - step), (lane >= step, step)):
            keeps.append((keep.astype(jnp.float32), by))
            count = count + keeps[-1][0]
    share = 1.0 / count
    window = lax.broadcasted_iota(jnp.int32, (gap_mask.shape[0], wide), 1) // bin_count
    spread = window == lax.broadcasted_iota(jnp.int32, window.shape, 0)
    spread = spread.astype(jnp.float32).astype(jnp.bfloat16)
    copies[0].wait()
    kept = lax.dot_general(
        gap_mask[...].astype(jnp.float32).astype(jnp.bfloat16),
        spread,
        (((0,), (0,)), ((), ())),
        preferred_element_type=jnp.float32,
    )
    copies[1].wait()
    real = spectra[0].astype(jnp.float32)
    imag = spectra[1].astype(jnp.float32)
    amplitude = jnp.sqrt(real * real + imag * imag)
    rows = (amplitude.shape[0] // 8, 1)
    total = amplitude
    for keep, by in keeps:
        total = total + jnp.tile(keep, rows) * pltpu.roll(amplitude, by, 1)
    level = jnp.maximum(total * jnp.tile(share, rows), level_floor)
    factor = kept / level
    out[:, :wide] = (real * factor).astype(jnp.bfloat16)
    out[:, wide:] = (imag * factor).astype(jnp.bfloat16)
    copies[2].wait()


def whiten(spectra, gap_mask):
    members, wide = spectra.shape[1:]
    win_count = gap_mask.shape[1]
    tables = phase_tables(wide // win_count, win_count, LAGS)
    vmem = pl.BlockSpec(memory_space=pltpu.VMEM)
    anywhere = pl.BlockSpec(memory_space=pl.ANY)
    return pl.pallas_call(
        whiten_body,
        out_shape=[
            pltpu.VMEM((members, 2 * wide), jnp.bfloat16),
            pltpu.VMEM(tables.shape, jnp.float32),
        ],
        in_specs=[anywhere] * 3,
        out_specs=[vmem] * 2,
        scratch_shapes=[
            pltpu.VMEM(spectra.shape, spectra.dtype),
            pltpu.VMEM((win_count, members), gap_mask.dtype),
            pltpu.SemaphoreType.DMA((3,)),
        ],
        compiler_params=pltpu.CompilerParams(vmem_limit_bytes=ROOM),
        name="whiten",
    )(far(spectra), far(gap_mask.T), far(tables))


def modulate_body(white, tables, out):
    members = white.shape[0]
    wide = white.shape[1] // 2
    real = white[:, :wide].astype(jnp.float32)
    imag = white[:, wide:].astype(jnp.float32)
    lags = tables.shape[0] // 2
    for lag in range(lags):
        rows = slice(lag * members, (lag + 1) * members)
        c = tables[lag : lag + 1, :]
        s = tables[lags + lag : lags + lag + 1, :]
        out[rows, :wide] = (c * real - s * imag).astype(jnp.bfloat16)
        out[rows, wide:] = (c * imag + s * real).astype(jnp.bfloat16)


def modulate(white, tables):
    members = white.shape[0]
    return pl.pallas_call(
        modulate_body,
        out_shape=pltpu.VMEM((LAGS * members, white.shape[1]), jnp.bfloat16),
        compiler_params=pltpu.CompilerParams(vmem_limit_bytes=ROOM),
        cost_estimate=pl.CostEstimate(flops=12 * LAGS * white.size, bytes_accessed=0, transcendentals=0),
        name="modulate",
    )(near(white), near(tables))


def walk_at(seat, chips):
    return jnp.where(seat < chips // 2, 2 * seat, 2 * (chips - 1 - seat) + 1)


def seat_of(chip, chips):
    return jnp.where(chip % 2 == 0, chip // 2, chips - 1 - chip // 2)


def correlate(modulated, groups, chips, shape, before, end):
    members = shape[1]
    count = len(groups)
    flat = [piece for _, mine, other in groups for piece in (mine, other)]
    old_groups, old_tiles, onto = before if before else ([], None, None)
    olds = ([] if old_tiles is None else [old_tiles]) + ([] if onto is None else [onto])

    def body(modulated, *rest):
        pieces = rest[: len(flat)]
        old_tile = rest[len(flat)]
        tail = rest[len(flat) + len(olds) :]
        if end:
            out, block, sems, tile = tail
        elif old_groups:
            tile, out, block, sems = tail
        else:
            tile, block, sems = tail
        place = lax.axis_index("blk")
        core = lax.rem(place, 2)
        seat = seat_of(lax.div(place, 2), chips)
        copies = []

        def send(source, back, some, sem):
            home = walk_at(lax.rem(seat + chips - back * (1 - 2 * core), chips), chips)
            columns = pl.ds(pl.multiple_of(home * (2 * members), 2 * members), 2 * members)
            copy = pltpu.make_async_copy(source, out.at[some, :, columns], sem)
            copy.start()
            copies.append(copy)

        for g, (back, _, _) in enumerate(old_groups):
            send(old_tile.at[g], back, slice(None), sems.at[g, PARTS])
        for g in range(count):
            for side, piece in ((core, pieces[2 * g]), (1 - core, pieces[2 * g + 1])):
                rows = pl.ds(pl.multiple_of((2 * g + side) * members, members), members)
                block[rows, :] = piece[...]
        parts = PARTS if end else 1
        lags = shape[0] // parts
        for part in range(parts):
            some = pl.ds(part * lags, lags)
            sums = lax.dot_general(
                modulated[part * lags * members : (part + 1) * lags * members, :],
                block[...],
                (((1,), (1,)), ((), ())),
                preferred_element_type=jnp.float32,
            ).reshape(lags, members, 2 * count * members)
            for g, (back, _, _) in enumerate(groups):
                tile[g, some] = sums[:, :, 2 * g * members : 2 * (g + 1) * members]
                if end:
                    send(tile.at[g, some], back, some, sems.at[g, part])
        for copy in copies:
            copy.wait()

    vmem = pl.BlockSpec(memory_space=pltpu.VMEM)
    anywhere = pl.BlockSpec(memory_space=pl.ANY)
    tile_shape = (count, shape[0], members, 2 * members)
    outs = [] if end else [(pltpu.VMEM(tile_shape, jnp.float32), vmem)]
    if old_groups:
        outs.append((jax.ShapeDtypeStruct(shape, jnp.float32), anywhere))
    scratch = [
        pltpu.VMEM((count * 2 * members, modulated.shape[1]), jnp.bfloat16),
        pltpu.SemaphoreType.DMA((max(count, len(old_groups)), PARTS + 1)),
    ]
    got = pl.pallas_call(
        body,
        out_shape=[shaped for shaped, _ in outs],
        in_specs=[vmem] * (1 + len(flat)) + [vmem] * (old_tiles is not None) + [anywhere] * (onto is not None),
        out_specs=[spec for _, spec in outs],
        scratch_shapes=scratch + ([pltpu.VMEM(tile_shape, jnp.float32)] if end else []),
        input_output_aliases={} if onto is None else {2 + len(flat): len(outs) - 1},
        compiler_params=pltpu.CompilerParams(vmem_limit_bytes=ROOM),
        cost_estimate=pl.CostEstimate(
            flops=4 * count * members * modulated.size, bytes_accessed=0, transcendentals=0
        ),
        name="correlate",
    )(
        near(modulated),
        *[near(piece) for piece in flat],
        *([] if old_tiles is None else [near(old_tiles)]),
        *([] if onto is None else [onto]),
    )
    if end:
        return got[0]
    return groups, got[0], got[1] if old_groups else None


def per_device(spectra, gap_mask):
    devices = lax.axis_size("blk")
    chips = devices // 2
    walk = list(range(0, chips, 2)) + list(range(1, chips, 2))[::-1]
    members = spectra.shape[1]
    shape = (LAGS, members, devices * members)

    def onward(array, step):
        pairs = [
            (2 * walk[i] + (c + step + 1) % 2, 2 * walk[(i + 1 - 2 * c) % chips] + (c + step) % 2)
            for i in range(chips)
            for c in range(2)
        ]
        return lax.ppermute(array, "blk", pairs)

    def swap(array):
        return lax.ppermute(array, "blk", [(i, i ^ 1) for i in range(devices)])

    def add(groups, before, end=False):
        return correlate(modulated, groups, chips, shape, before, end)

    white, tables = whiten(spectra, gap_mask)
    modulated = modulate(white, tables)

    mine, other = white, swap(white)
    out = add([(0, mine, other)], None)
    final = chips // 2
    for step in range(1, final):
        mine = onward(mine, step)
        other = onward(other, step)
        mine_there, other_there = swap(mine), swap(other)
        if step % 2:
            groups = [(-step, other, mine), (step, mine_there, other_there)]
        else:
            groups = [(step, mine, other), (-step, other_there, mine_there)]
        out = add(groups, out)
    last = onward(mine, final)
    there = swap(last)
    return add([(final, there, last) if final % 2 else (final, last, there)], out, end=True)


def solution(mesh):
    placed = (P(None, ("group", "blk"), None), P(("group", "blk"), None))
    return jax.shard_map(
        per_device,
        mesh=mesh,
        in_specs=placed,
        out_specs=P(None, ("group", "blk"), None),
        check_vma=False,
    )
```
